256 devices in a mesh: face: 16 (over z, core), sub: 16 (over y, x).
Axes of the slice: x: 4, y: 4, z: 8, core: 2. Of those that a mesh axis runs over, the one named last changes fastest.
Arguments:
- mesh_latent: bfloat16 [65536, 512], P(('face', 'sub')), may hold values from -6 to 6
- edge_latent: bfloat16 [524288, 512], P(('face', 'sub')), may hold values from -6 to 6
- grid_features: bfloat16 [65536, 384], P(('face', 'sub')), may hold values from -6 to 6
- senders: int32 [524288], P(('face', 'sub')), may hold values from 0 to 383, as said below
- receivers: int32 [524288], P(('face', 'sub')), may hold values from 0 to 255
- send_lists: int32 [256, 4, 32], P(('face', 'sub')), may hold values from -1 to 255, as said below
- link_sources: int32 [131072], P(('face', 'sub')), may hold values from 0 to 255
- link_targets: int32 [131072], P(('face', 'sub')), may hold values from 0 to 255
- node_area: float32 [65536], P(('face', 'sub')), may hold values from 0.25 to 4.5
- grid_weight: bfloat16 [384, 512], P(None, 'sub'), may hold values from -0.3125 to 0.3125
- encode_weight: bfloat16 [1024, 512], P('sub'), may hold values from -0.1875 to 0.1875
- edge_first: bfloat16 [1, 1536, 512], P(None, 'sub'), may hold values from -0.15625 to 0.15625
- edge_second: bfloat16 [1, 512, 512], P(None, 'sub'), may hold values from -0.25 to 0.25
- node_first: bfloat16 [1, 1024, 512], P(None, 'sub'), may hold values from -0.1875 to 0.1875
- node_second: bfloat16 [1, 512, 512], P(None, 'sub'), may hold values from -0.25 to 0.25
Outputs:
- mesh_result: bfloat16 [65536, 512], P(('face', 'sub'))
- edge_result: bfloat16 [524288, 512], P(('face', 'sub'))
- masses: float32 [1, 512], replicated
The draws below stay inside these ranges and needn't reach their ends.
Inputs may be any that keep to these rules, and one draw needn't show every extreme that they name: `send_lists`: entries are the sending partition's own node numbers, or -1 for an unused slot; in every list the used slots come first, hold distinct nodes and number 32 // 2 or more; for every list number some partition uses all 32 slots. `senders`: A value below 256 names one of the partition's own nodes; 256 + d * 32 + k names slot k of the list with number d that the partition receives, and that slot is always a used one.
All inputs are finite; a program needn't handle non-finite values.
Results may differ from the reference program's by a relative error of at most 0.008.
Values may be sent and summed in bfloat16 or wider, within the bound.
A program may use at most 64 MiB of HBM per device.

```python
import jax
import jax.numpy as jnp
from jax import lax

D = 512
GFEAT = 384
NODE_DEV = 256
EDGE_DEV = 2048
GRID_DEV = 256
LINK_DEV = 512
HALO = 32
LAYERS = 1
NODES = 65536
EDGES = 524288
GRIDS = 65536
LINKS = 131072
N_FACE = 16
N_SUB = 16


def halo_live(key):
    partitions = N_FACE * N_SUB
    first_key, second_key = jax.random.split(jax.random.fold_in(key, 11))
    live_count = jax.random.randint(first_key, (partitions, 4), HALO // 2, HALO + 1)
    full_device = jax.random.randint(second_key, (4,), 0, partitions)
    live_count = jnp.where(jnp.arange(partitions)[:, None] == full_device[None, :], HALO, live_count)
    return live_count.astype(jnp.int32)


def draw_send_lists(key, part):
    partitions = N_FACE * N_SUB
    live_count = halo_live(key)
    scores = jax.random.randint(jax.random.fold_in(key, 12), (partitions, 4, NODE_DEV), 0, 1 << 20)
    scores = scores * NODE_DEV + jnp.arange(NODE_DEV, dtype=jnp.int32)[None, None, :]
    ranking = jnp.argsort(scores, axis=-1).astype(jnp.int32)[:, :, :HALO]
    slot_index = jnp.arange(HALO, dtype=jnp.int32)
    return jnp.where(slot_index[None, None, :] < live_count[:, :, None], ranking, -1).astype(jnp.int32)


def draw_senders(key, part):
    partitions = N_FACE * N_SUB
    live_count = halo_live(key)
    first_key, second_key, third_key, fourth_key = jax.random.split(jax.random.fold_in(key, 13), 4)
    total = partitions * EDGE_DEV
    device_of = jnp.arange(total, dtype=jnp.int32) // EDGE_DEV
    face_index = device_of // N_SUB
    sub_index = device_of % N_SUB
    direction = jax.random.randint(first_key, (total,), 0, 4)
    source = jnp.where(direction == 0, (face_index - 1) % N_FACE * N_SUB + sub_index, jnp.where(direction == 1, (face_index + 1) % N_FACE * N_SUB + sub_index, jnp.where(direction == 2, face_index * N_SUB + (sub_index - 1) % N_SUB, face_index * N_SUB + (sub_index + 1) % N_SUB)))
    live_here = live_count[source, direction]
    slot_index = jax.random.randint(second_key, (total,), 0, 1 << 20) % live_here
    remote = NODE_DEV + direction * HALO + slot_index
    local_node = jax.random.randint(third_key, (total,), 0, NODE_DEV)
    use_halo = jax.random.randint(fourth_key, (total,), 0, 4) == 0
    return jnp.where(use_halo, remote, local_node).astype(jnp.int32)


def draw_node_area(key, part):
    ramp_scale = 1.0 + 2.0 * jnp.arange(NODES, dtype=jnp.float32) / NODES
    factor = jax.random.uniform(key, (NODES,), jnp.float32, 0.5, 1.5)
    return (ramp_scale * factor).astype(jnp.float32)


def place_ends(drawn, stream_key, low, high):
    index_at = [jax.random.randint(jax.random.fold_in(stream_key, axis), (), 0, length) for axis, length in enumerate(drawn.shape)]
    main_axis = drawn.shape.index(max(drawn.shape))
    neighbour = index_at[:main_axis] + [(index_at[main_axis] + 1) % drawn.shape[main_axis]] + index_at[main_axis + 1:]
    return drawn.at[tuple(index_at)].set(low).at[tuple(neighbour)].set(high)


def shard_levels(key, extent, cuts, smallest, largest):
    def one(axis_at, parts):
        draws = jax.random.uniform(jax.random.fold_in(jax.random.fold_in(key, 6), axis_at), (parts,), jnp.float32, smallest / len(cuts), largest / len(cuts))
        return jnp.repeat(jnp.exp(draws), extent[axis_at] // parts).reshape((-1,) + (1,) * (len(extent) - axis_at - 1))

    factor_of = one(*cuts[0])
    for cut in cuts[1:]:
        factor_of = factor_of * one(*cut)
    return factor_of


def centred(own_key, shape, deviation, limit, cuts=(), kind=jnp.bfloat16):
    gain = shard_levels(own_key, shape, cuts, -0.22, 0.18) if cuts else 1.0
    result = jax.random.normal(own_key, shape, jnp.float32) * deviation * gain
    return jnp.minimum(jnp.maximum(result, -limit), limit).astype(kind)


def setup_inputs(seed: int = 0) -> dict:
    key_of = jax.random.split(jax.random.key(seed), 16)
    return {
        "mesh_latent": centred(key_of[0], (NODES, D), 1.0, 6.0, ((0, 256),)),
        "edge_latent": centred(key_of[1], (EDGES, D), 1.0, 6.0, ((0, 256),)),
        "grid_features": centred(key_of[2], (GRIDS, GFEAT), 1.0, 6.0, ((0, 256),)),
        "senders": draw_senders(jax.random.fold_in(key_of[15], 71), 0),
        "receivers": place_ends(jax.random.randint(key_of[4], (EDGES,), 0, NODE_DEV), jax.random.fold_in(key_of[4], 1), 0, NODE_DEV - 1).astype(jnp.int32),
        "send_lists": draw_send_lists(jax.random.fold_in(key_of[15], 71), 0),
        "link_sources": place_ends(jax.random.randint(key_of[6], (LINKS,), 0, GRID_DEV), jax.random.fold_in(key_of[6], 1), 0, GRID_DEV - 1).astype(jnp.int32),
        "link_targets": place_ends(jax.random.randint(key_of[7], (LINKS,), 0, NODE_DEV), jax.random.fold_in(key_of[7], 1), 0, NODE_DEV - 1).astype(jnp.int32),
        "node_area": draw_node_area(jax.random.fold_in(key_of[15], 71), 0),
        "grid_weight": centred(key_of[9], (GFEAT, D), GFEAT ** -0.5, 0.3125, ((1, 16),)),
        "encode_weight": centred(key_of[10], (2 * D, D), (2 * D) ** -0.5, 0.1875, ((0, 16),)),
        "edge_first": centred(key_of[11], (LAYERS, 3 * D, D), (3 * D) ** -0.5, 0.15625, ((1, 16),)),
        "edge_second": centred(key_of[12], (LAYERS, D, D), D ** -0.5, 0.25, ((1, 16),)),
        "node_first": centred(key_of[13], (LAYERS, 2 * D, D), (2 * D) ** -0.5, 0.1875, ((1, 16),)),
        "node_second": centred(key_of[14], (LAYERS, D, D), D ** -0.5, 0.25, ((1, 16),)),
    }


def global_slots(send_lists):
    partitions = N_FACE * N_SUB
    part_ids = jnp.arange(partitions, dtype=jnp.int32)
    face_index = part_ids // N_SUB
    sub_index = part_ids % N_SUB
    sources = jnp.stack([((face_index - 1) % N_FACE) * N_SUB + sub_index,
                         ((face_index + 1) % N_FACE) * N_SUB + sub_index,
                         face_index * N_SUB + (sub_index - 1) % N_SUB,
                         face_index * N_SUB + (sub_index + 1) % N_SUB], axis=1).astype(jnp.int32)
    incoming_lists = send_lists[sources, jnp.arange(4, dtype=jnp.int32)[None, :], :]
    remote = jnp.where(incoming_lists >= 0, sources[:, :, None] * NODE_DEV + incoming_lists, NODES)
    own_rows = part_ids[:, None] * NODE_DEV + jnp.arange(NODE_DEV, dtype=jnp.int32)[None, :]
    return jnp.concatenate([own_rows, remote.reshape(partitions, 4 * HALO).astype(jnp.int32)], axis=1).astype(jnp.int32)


def reference(mesh_latent, edge_latent, grid_features, senders, receivers, send_lists, link_sources, link_targets, node_area, grid_weight, encode_weight, edge_first, edge_second, node_first, node_second):
    partitions = N_FACE * N_SUB
    grid_latent = jax.nn.silu(jnp.dot(grid_features, grid_weight, preferred_element_type=jnp.float32)).astype(jnp.bfloat16)

    def encode_block(block):
        grid_rows, node_rows, sources, targets = block
        joined = jnp.concatenate([jnp.take(grid_rows, sources, axis=0), jnp.take(node_rows, targets, axis=0)], axis=1)
        messages = jax.nn.silu(jnp.dot(joined, encode_weight, preferred_element_type=jnp.float32)).astype(jnp.bfloat16)
        return jax.ops.segment_sum(messages.astype(jnp.float32), targets, num_segments=NODE_DEV)

    gathered = lax.map(encode_block, (grid_latent.reshape(partitions, GRID_DEV, D),
                                      mesh_latent.reshape(partitions, NODE_DEV, D),
                                      link_sources.reshape(partitions, LINK_DEV),
                                      link_targets.reshape(partitions, LINK_DEV)))
    latent = (mesh_latent.astype(jnp.float32) + gathered.reshape(NODES, D)).astype(jnp.bfloat16)

    slot_table = global_slots(send_lists)
    offsets = (jnp.arange(partitions, dtype=jnp.int32) * NODE_DEV)[:, None]
    local_receivers = receivers.reshape(partitions, EDGE_DEV)
    global_receivers = (local_receivers + offsets).astype(jnp.int32)
    edge_senders = senders.reshape(partitions, EDGE_DEV)
    edge_state = edge_latent.reshape(partitions, EDGE_DEV, D)
    totals = []
    for layer_index in range(LAYERS):
        padded = jnp.concatenate([latent, jnp.zeros((1, D), jnp.bfloat16)], axis=0)
        first_weight = edge_first[layer_index]
        second_weight = edge_second[layer_index]

        def edge_block(block):
            edges, slots, sends, global_recv, local_recv = block
            joined = jnp.concatenate([edges, jnp.take(padded, jnp.take(slots, sends), axis=0),
                                      jnp.take(latent, global_recv, axis=0)], axis=1)
            hidden = jax.nn.silu(jnp.dot(joined, first_weight, preferred_element_type=jnp.float32)).astype(jnp.bfloat16)
            updated = (edges.astype(jnp.float32) + jnp.dot(hidden, second_weight, preferred_element_type=jnp.float32)).astype(jnp.bfloat16)
            incoming = jax.ops.segment_sum(updated.astype(jnp.float32), local_recv, num_segments=NODE_DEV)
            return updated, incoming

        edge_state, incoming = lax.map(edge_block, (edge_state, slot_table, edge_senders, global_receivers, local_receivers))
        incoming = incoming.reshape(NODES, D).astype(jnp.bfloat16)
        node_hidden = jax.nn.silu(jnp.dot(jnp.concatenate([latent, incoming], axis=1), node_first[layer_index],
                                          preferred_element_type=jnp.float32)).astype(jnp.bfloat16)
        latent = (latent.astype(jnp.float32) + jnp.dot(node_hidden, node_second[layer_index],
                                                       preferred_element_type=jnp.float32)).astype(jnp.bfloat16)
        totals.append(jnp.dot(node_area, latent.astype(jnp.float32), precision=lax.Precision.HIGHEST))
    masses = jnp.stack(totals) / NODES
    return latent, edge_state.reshape(EDGES, D), masses
```

```python
import functools

import jax
import jax.numpy as jnp
from jax import lax
from jax.experimental import pallas as pl
from jax.experimental.pallas import tpu as pltpu
from jax.sharding import PartitionSpec as P

BF = jnp.bfloat16
F32 = jnp.float32
MESH = pl.DeviceIdType.MESH

GRID_AT, ENC_AT, EF_AT, ES_AT, NF_AT, NS_AT, ROWS = 0, 16, 48, 96, 112, 144, 160
GROUPS = ((0, 48), (48, 96), (96, 160))
TILE = 512


def silu(v):
    h = 0.5 * v
    return h + h * jnp.tanh(h)


def dot(a, b):
    return jnp.dot(a, b, preferred_element_type=F32)


def column(row):
    return jnp.broadcast_to(row, (128, 128)).T


def kernel(
    mesh_h, edge_h, gridf_h, snd_h, rcv_h, lists_h, lsrc_h, ltgt_h, area_h,
    gw_h, enc_h, ef_h, es_h, nf_h, ns_h,
    mesh_o, edge_o, mass_o,
    buf, gs, mesh_v, gridf_v, x_v, snd_v, rcv_v, lists_v, lsrc_v, ltgt_v, area_v,
    gt_w, enc_w, r_w, w23, es_w, nf_w, ns_w,
    ol, olt, ort, e1, new_v, l0, res_v, hs, hr, acol, msrc, asub, fsrc, aface,
    in_sem, w_sem, out_sem,
    p1_s, p1_r, p1f_s, p1f_r, p2_s, p2_r, p2f_s, p2f_r, dd_s, dd_r,
    h_s, h_r, ms_s, ms_r, mf_s, mf_r,
):
    f = lax.axis_index("face")
    s = lax.axis_index("sub")
    c = lax.rem(f, 2)
    y, x = lax.div(s, 4), lax.rem(s, 4)
    b = y + c * (x - y)
    a = x + c * (y - x)
    wa, wb = 1 + 3 * c, 4 - 3 * c
    a_r, a_l, a_2 = lax.rem(a + 1, 4), lax.rem(a + 3, 4), lax.rem(a + 2, 4)
    b_r, b_l, b_2 = lax.rem(b + 1, 4), lax.rem(b + 3, 4), lax.rem(b + 2, 4)
    to_ar, to_al = (f, b * wb + a_r * wa), (f, b * wb + a_l * wa)
    to_br, to_bl = (f, b_r * wb + a * wa), (f, b_l * wb + a * wa)
    sibling = (f + 1 - 2 * c, s)
    other = 1 - c

    loads = []
    for at, rows, ref in (
        (ENC_AT, 32, enc_h), (EF_AT, 48, ef_h), (ES_AT, 16, es_h), (NF_AT, 32, nf_h), (NS_AT, 16, ns_h),
    ):
        n = len(loads)
        loads.append(pltpu.make_async_copy(
            ref.at[pl.ds(c * rows, rows)], buf.at[c, b, a, pl.ds(at, rows)], w_sem.at[n]))
        loads.append(pltpu.make_async_copy(
            ref.at[pl.ds(other * rows, rows)], buf.at[other, a, b, pl.ds(at, rows)], w_sem.at[n + 1]))
    gload = pltpu.make_async_copy(gw_h, gs, w_sem.at[10])
    gload.start()
    for copy in loads:
        copy.start()
    ins = [
        pltpu.make_async_copy(src, dst, in_sem.at[n])
        for n, (src, dst) in enumerate((
            (lsrc_h, lsrc_v), (ltgt_h, ltgt_v), (snd_h, snd_v), (rcv_h, rcv_v), (lists_h, lists_v),
            (area_h, area_v), (gridf_h, gridf_v), (mesh_h, mesh_v), (edge_h, x_v.at[:, pl.ds(0, 512)]),
        ))
    ]
    for copy in ins:
        copy.start()

    barrier = pltpu.get_barrier_semaphore()
    for k in range(1, 16):
        pl.semaphore_signal(barrier, inc=1, device_id=(f, lax.rem(s + k, 16)), device_id_type=MESH)
        pl.semaphore_signal(barrier, inc=1, device_id=(lax.rem(f + k, 16), s), device_id_type=MESH)

    gload.wait()
    turned = gs[...].astype(F32).T.astype(BF)
    first, second = turned[0:16], turned[16:32]
    mine = jnp.where(c == 0, first, second)
    theirs = jnp.where(c == 0, second, first)
    pad = jnp.zeros((16, 128), BF)
    buf[c, b, a, 0:16, :] = jnp.concatenate([mine, pad], axis=1)
    buf[other, a, b, 0:16, :] = jnp.concatenate([theirs, pad], axis=1)
    for copy in loads:
        copy.wait()

    pl.semaphore_wait(barrier, 30)

    def remote(src, dst, send, recv, to):
        copy = pltpu.make_async_remote_copy(
            src_ref=src, dst_ref=dst, send_sem=send, recv_sem=recv, device_id=to, device_id_type=MESH)
        return copy

    def same(ref, send, recv, to):
        return remote(ref, ref, send, recv, to)

    p1, p1f, p2, p2f, dd = [], [], [], [], []
    for g, (lo, hi) in enumerate(GROUPS):
        rows = pl.ds(lo, hi - lo)
        p1.append([
            same(buf.at[c, b, a, rows], p1_s.at[g, 0], p1_r.at[g, 0], to_ar),
            same(buf.at[c, b, a, rows], p1_s.at[g, 1], p1_r.at[g, 1], to_al),
        ])
        left, right = pl.ds(0, 256), pl.ds(256, 256)
        p1f.append([
            same(buf.at[c, b, a_l, rows, left], p1f_s.at[g, 0], p1f_r.at[g, 0], to_ar),
            same(buf.at[c, b, a_r, rows, right], p1f_s.at[g, 1], p1f_r.at[g, 1], to_al),
        ])
        every = pl.ds(0, 4)
        p2.append([
            same(buf.at[c, b, every, rows], p2_s.at[g, 0], p2_r.at[g, 0], to_br),
            same(buf.at[c, b, every, rows], p2_s.at[g, 1], p2_r.at[g, 1], to_bl),
        ])
        p2f.append([
            same(buf.at[c, b_l, pl.ds(0, 2), rows], p2f_s.at[g, 0], p2f_r.at[g, 0], to_br),
            same(buf.at[c, b_r, pl.ds(2, 2), rows], p2f_s.at[g, 1], p2f_r.at[g, 1], to_bl),
        ])
        dd.append([
            same(buf.at[c, b, a_l, rows], dd_s.at[g, 0], dd_r.at[g, 0], sibling),
            same(buf.at[c, b, a_r, rows], dd_s.at[g, 1], dd_r.at[g, 1], sibling),
            same(buf.at[c, b, a_2, rows], dd_s.at[g, 2], dd_r.at[g, 2], sibling),
            same(buf.at[c, b_l, every, rows], dd_s.at[g, 3], dd_r.at[g, 3], sibling),
            same(buf.at[c, b_r, every, rows], dd_s.at[g, 4], dd_r.at[g, 4], sibling),
            same(buf.at[c, b_2, every, rows], dd_s.at[g, 5], dd_r.at[g, 5], sibling),
        ])

    def start(copies):
        for copy in copies:
            copy.start()

    def arrived(copies):
        for copy in copies:
            copy.wait_recv()

    def pass_p1(g):
        arrived(p1[g])
        start(p1f[g])
        start(dd[g][0:2])

    def pass_p1f(g):
        arrived(p1f[g])
        start(p2[g])
        start(dd[g][2:3])

    def pass_p2(g):
        arrived(p2[g])
        start(p2f[g])
        start(dd[g][3:5])

    def pass_p2f(g):
        arrived(p2f[g])
        start(dd[g][5:6])

    for g in range(3):
        start(p1[g])

    for copy in ins[0:6]:
        copy.wait()
    lanes = lax.broadcasted_iota(jnp.int32, (128, 128), 1).astype(F32)
    node_rows = lax.broadcasted_iota(jnp.int32, (256, 128), 0).astype(F32)

    def hot(col, first):
        return jnp.where(col == lanes + float(first), 1.0, 0.0).astype(BF)

    pass_p1(0)
    pass_p1(1)
    pass_p1(2)
    lsrc = lsrc_v[...].astype(F32)
    ltgt = ltgt_v[...].astype(F32)
    for j in range(4):
        col = column(lsrc[j:j + 1])
        for k in range(2):
            ol[128 * j:128 * (j + 1), 128 * k:128 * (k + 1)] = hot(col, 128 * k)
        col = column(ltgt[j:j + 1])
        for k in range(2):
            ol[128 * j:128 * (j + 1), 256 + 128 * k:256 + 128 * (k + 1)] = hot(col, 128 * k)
        olt[:, 128 * j:128 * (j + 1)] = jnp.where(node_rows == ltgt[j:j + 1], 1.0, 0.0).astype(BF)
    pass_p1f(0)
    pass_p1f(1)

    snd = snd_v[...].astype(F32)
    rcv = rcv_v[...].astype(F32)

    def edge_hot(js):
        for j in js:
            at = slice(128 * j, 128 * (j + 1))
            col = column(snd[j:j + 1])
            for k in range(2):
                x_v[at, 512 + 128 * k:512 + 128 * (k + 1)] = hot(col, 128 * k)
            x_v[at, 1024:1152] = hot(col, 256)
            col = column(rcv[j:j + 1])
            for k in range(2):
                x_v[at, 768 + 128 * k:768 + 128 * (k + 1)] = hot(col, 128 * k)
            t, o = j // 4, 128 * (j % 4)
            ort[t, :, o:o + 128] = jnp.where(node_rows == rcv[j:j + 1], 1.0, 0.0).astype(BF)

    edge_hot(range(0, 8))
    for j in range(2):
        acol[128 * j:128 * (j + 1), :] = column(area_v[j:j + 1, :])
    pass_p2(0)
    pass_p1f(2)
    edge_hot(range(8, 16))
    pass_p2f(0)
    pass_p2(1)

    def assemble(at, rows, put):
        for i in range(16):
            put(i * 2 * rows, buf[0, i // 4, i % 4, at:at + rows, :])
            put(i * 2 * rows + rows, buf[1, i % 4, i // 4, at:at + rows, :])

    arrived(dd[0])
    for i in range(16):
        gt_w[i * 32:i * 32 + 16, :] = buf[0, i // 4, i % 4, 0:16, 0:384]
        gt_w[i * 32 + 16:i * 32 + 32, :] = buf[1, i % 4, i // 4, 0:16, 0:384]

    def put_enc(at, block):
        enc_w[at:at + block.shape[0], :] = block

    assemble(ENC_AT, 32, put_enc)
    for copy in ins[6:9]:
        copy.wait()

    grid_latent = silu(lax.dot_general(
        gridf_v[...], gt_w[...], (((1,), (1,)), ((), ())), preferred_element_type=F32)).astype(BF)
    from_grid = dot(grid_latent, enc_w[0:512, :]).astype(BF)
    from_mesh = dot(mesh_v[...], enc_w[512:1024, :]).astype(BF)
    messages = silu(dot(ol[...], jnp.concatenate([from_grid, from_mesh], axis=0))).astype(BF)
    l0[...] = (mesh_v[...].astype(F32) + dot(olt[...], messages)).astype(BF)

    slot_rows = lax.broadcasted_iota(jnp.int32, (256, 32), 0)
    for d in range(4):
        pick = jnp.where(slot_rows == lists_v[d:d + 1, :], 1.0, 0.0).astype(BF)
        hs[d] = lax.dot_general(
            pick, l0[...], (((0,), (0,)), ((), ())), preferred_element_type=F32).astype(BF)
    targets = (
        (lax.rem(f + 1, 16), s), (lax.rem(f + 15, 16), s), (f, lax.rem(s + 1, 16)), (f, lax.rem(s + 15, 16)))
    halo = [remote(hs.at[d], hr.at[d], h_s.at[d], h_r.at[d], targets[d]) for d in range(4)]
    start(halo)
    pass_p2f(1)
    pass_p2(2)
    arrived(dd[1])

    def put_ef(at, block):
        done = 0
        while done < block.shape[0]:
            place = at + done
            limit = block.shape[0] - done if place >= 512 else min(block.shape[0] - done, 512 - place)
            if place < 512:
                r_w[place:place + limit, :] = block[done:done + limit]
            else:
                w23[place - 512:place - 512 + limit, :] = block[done:done + limit]
            done += limit

    assemble(EF_AT, 48, put_ef)
    r_w[512:768, :] = dot(l0[...], w23[0:512, :]).astype(BF)
    r_w[768:1024, :] = dot(l0[...], w23[512:1024, :]).astype(BF)
    for t in range(4):
        at = slice(TILE * t, TILE * (t + 1))
        e1[at, :] = dot(x_v[at, 0:1024], r_w[0:1024, :])
        if t == 1:
            pass_p2f(2)
    arrived(halo)
    r_w[1024:1152, :] = dot(hr[...].reshape(128, 512), w23[0:512, :]).astype(BF)
    arrived(dd[2])

    def put_to(ref):
        def put(at, block):
            ref[at:at + block.shape[0], :] = block
        return put

    assemble(ES_AT, 16, put_to(es_w))

    writes = []
    incoming = jnp.zeros((256, 512), F32)
    for t in range(4):
        at = slice(TILE * t, TILE * (t + 1))
        hidden = silu(e1[at, :] + dot(x_v[at, 1024:1152], r_w[1024:1152, :])).astype(BF)
        new = (x_v[at, 0:512].astype(F32) + dot(hidden, es_w[...])).astype(BF)
        new_v[at, :] = new
        write = pltpu.make_async_copy(new_v.at[pl.ds(TILE * t, TILE)], edge_o.at[pl.ds(TILE * t, TILE)], out_sem.at[t])
        write.start()
        writes.append(write)
        incoming = incoming + dot(ort[t], new)
    assemble(NF_AT, 32, put_to(nf_w))
    assemble(NS_AT, 16, put_to(ns_w))

    node_hidden = silu(dot(l0[...], nf_w[0:512, :]) + dot(incoming.astype(BF), nf_w[512:1024, :])).astype(BF)
    result = (l0[...].astype(F32) + dot(node_hidden, ns_w[...])).astype(BF)
    res_v[...] = result
    write = pltpu.make_async_copy(res_v, mesh_o, out_sem.at[4])
    write.start()
    writes.append(write)

    wide = result.astype(F32)
    msrc[...] = jnp.zeros((8, 128), F32)
    for k in range(4):
        msrc[k:k + 1, :] = jnp.sum(wide[:, 128 * k:128 * (k + 1)] * acol[...], axis=0, keepdims=True)

    def exchange(source, slots, me, peer, sends, recvs):
        slots[me] = source[...]
        copies = [
            remote(source, slots.at[me], sends.at[k - 1], recvs.at[me], peer(lax.rem(me + k, 16)))
            for k in range(1, 16)
        ]
        start(copies)
        for k in range(1, 16):
            j = lax.rem(me + k, 16)
            remote(source, slots.at[j], sends.at[k - 1], recvs.at[j], peer(j)).wait_recv()
        return copies

    by_sub = exchange(msrc, asub, s, lambda j: (f, j), ms_s, ms_r)
    fsrc[...] = jnp.sum(asub[...], axis=0)
    by_face = exchange(fsrc, aface, f, lambda j: (j, s), mf_s, mf_r)
    total = jnp.sum(aface[...], axis=0) / 65536.0
    for k in range(4):
        mass_o[0:1, 128 * k:128 * (k + 1)] = total[k:k + 1, :]

    for copy in writes:
        copy.wait()
    for group in p1 + p1f + p2 + p2f + dd + [halo, by_sub, by_face]:
        for copy in group:
            copy.wait_send()


def per_device(
    mesh_latent, edge_latent, grid_features, senders, receivers, send_lists, link_sources, link_targets,
    node_area, grid_weight, encode_weight, edge_first, edge_second, node_first, node_second,
):
    dma = pltpu.SemaphoreType.DMA
    vm = pltpu.VMEM
    return pl.pallas_call(
        kernel,
        out_shape=(
            jax.ShapeDtypeStruct((256, 512), BF),
            jax.ShapeDtypeStruct((2048, 512), BF),
            jax.ShapeDtypeStruct((1, 512), F32),
        ),
        in_specs=[pl.BlockSpec(memory_space=pl.ANY)] * 15,
        out_specs=(
            pl.BlockSpec(memory_space=pl.ANY),
            pl.BlockSpec(memory_space=pl.ANY),
            pl.BlockSpec(memory_space=pltpu.VMEM),
        ),
        scratch_shapes=[
            vm((2, 4, 4, ROWS, 512), BF), vm((384, 32), BF), vm((256, 512), BF), vm((256, 384), BF),
            vm((2048, 1152), BF), vm((16, 128), jnp.int32), vm((16, 128), jnp.int32), vm((4, 32), jnp.int32),
            vm((4, 128), jnp.int32), vm((4, 128), jnp.int32), vm((2, 128), F32),
            vm((512, 384), BF), vm((1024, 512), BF), vm((1152, 512), BF), vm((1024, 512), BF),
            vm((512, 512), BF), vm((1024, 512), BF), vm((512, 512), BF),
            vm((512, 512), BF), vm((256, 512), BF), vm((4, 256, 512), BF), vm((2048, 512), F32),
            vm((2048, 512), BF), vm((256, 512), BF), vm((256, 512), BF), vm((4, 32, 512), BF),
            vm((4, 32, 512), BF), vm((256, 128), F32), vm((8, 128), F32), vm((16, 8, 128), F32),
            vm((8, 128), F32), vm((16, 8, 128), F32),
            dma((9,)), dma((11,)), dma((5,)),
            dma((3, 2)), dma((3, 2)), dma((3, 2)), dma((3, 2)), dma((3, 2)), dma((3, 2)), dma((3, 2)), dma((3, 2)),
            dma((3, 6)), dma((3, 6)), dma((4,)), dma((4,)),
            dma((15,)), dma((16,)), dma((15,)), dma((16,)),
        ],
        compiler_params=pltpu.CompilerParams(
            collective_id=0, has_side_effects=True, vmem_limit_bytes=60 * 1024 * 1024),
        cost_estimate=pl.CostEstimate(flops=6_000_000_000, bytes_accessed=6_000_000, transcendentals=1_500_000),
        name="graph_layer",
    )(
        mesh_latent, edge_latent, grid_features, senders.reshape(16, 128), receivers.reshape(16, 128),
        send_lists[0], link_sources.reshape(4, 128), link_targets.reshape(4, 128), node_area.reshape(2, 128),
        grid_weight, encode_weight, edge_first[0], edge_second[0], node_first[0], node_second[0],
    )


def solution(mesh):
    both = ("face", "sub")
    placed = (
        P(both, None), P(both, None), P(both, None), P(both), P(both), P(both, None, None), P(both), P(both), P(both),
        P(None, "sub"), P("sub", None), P(None, "sub", None), P(None, "sub", None), P(None, "sub", None),
        P(None, "sub", None),
    )
    return jax.shard_map(
        per_device, mesh=mesh, in_specs=placed, out_specs=(P(both, None), P(both, None), P()), check_vma=False)
```

```python
import functools

import jax
import jax.numpy as jnp
from jax import lax
from jax.experimental import pallas as pl
from jax.experimental.pallas import tpu as pltpu
from jax.sharding import PartitionSpec as P

BF = jnp.bfloat16
F32 = jnp.float32
MESH = pl.DeviceIdType.MESH

GRID_AT, ENC_AT, ES_AT, EF_AT, NF_AT, NS_AT, ROWS = 0, 16, 48, 64, 112, 144, 160
GROUPS = ((0, 64), (64, 112), (112, 160))
PIECES = 31
TILE = 512


def silu(v):
    h = 0.5 * v
    return h + h * jnp.tanh(h)


def dot(a, b):
    return jnp.dot(a, b, preferred_element_type=F32)


def column(row):
    return jnp.broadcast_to(row, (128, 128)).T


def kernel(
    mesh_h, edge_h, gridf_h, snd_h, rcv_h, lists_h, lsrc_h, ltgt_h, area_h,
    gw_h, enc_h, ef_h, es_h, nf_h, ns_h,
    mesh_o, edge_o, mass_o,
    buf, gs, mesh_v, gridf_v, x_v, snd_v, rcv_v, lists_v, lsrc_v, ltgt_v, area_v,
    gt_w, enc_w, r_w, w23, es_w, nf_w, ns_w,
    ol, olt, ort, e1, l0, hs, hr, acol, msrc, asub, fsrc, aface,
    in_sem, w_sem, g_s, g_r, near, far, h_s, h_r, ms_s, ms_r, mf_s, mf_r,
):
    f = lax.axis_index("face")
    s = lax.axis_index("sub")
    c = lax.rem(f, 2)
    y, x = lax.div(s, 4), lax.rem(s, 4)
    b = y + c * (x - y)
    a = x + c * (y - x)
    wa, wb = 1 + 3 * c, 4 - 3 * c
    a_r, a_l, a_2 = lax.rem(a + 1, 4), lax.rem(a + 3, 4), lax.rem(a + 2, 4)
    b_r, b_l, b_2 = lax.rem(b + 1, 4), lax.rem(b + 3, 4), lax.rem(b + 2, 4)
    to_ar, to_al = (f, b * wb + a_r * wa), (f, b * wb + a_l * wa)
    to_br, to_bl = (f, b_r * wb + a * wa), (f, b_l * wb + a * wa)
    sibling = (f + 1 - 2 * c, s)
    other = 1 - c
    z_r, z_l = lax.rem(f + 2, 16), lax.rem(f + 14, 16)
    z_2r, z_2l = lax.rem(f + 4, 16), lax.rem(f + 12, 16)

    loads = []
    for at, rows, ref in (
        (ENC_AT, 32, enc_h), (ES_AT, 16, es_h), (EF_AT, 48, ef_h), (NF_AT, 32, nf_h), (NS_AT, 16, ns_h),
    ):
        n = len(loads)
        loads.append(pltpu.make_async_copy(
            ref.at[pl.ds(c * rows, rows)], buf.at[c, b, a, pl.ds(at, rows)], w_sem.at[n]))
        loads.append(pltpu.make_async_copy(
            ref.at[pl.ds(other * rows, rows)], buf.at[other, a, b, pl.ds(at, rows)], w_sem.at[n + 1]))
    gload = pltpu.make_async_copy(gw_h, gs, w_sem.at[10])
    gload.start()
    for copy in loads:
        copy.start()
    ins = [
        pltpu.make_async_copy(src, dst, in_sem.at[n])
        for n, (src, dst) in enumerate((
            (lsrc_h, lsrc_v), (ltgt_h, ltgt_v), (snd_h, snd_v), (rcv_h, rcv_v), (lists_h, lists_v),
            (area_h, area_v), (gridf_h, gridf_v), (mesh_h, mesh_v), (edge_h, x_v.at[:, pl.ds(0, 512)]),
        ))
    ]
    for copy in ins:
        copy.start()

    barrier = pltpu.get_barrier_semaphore()
    for peer in (
        sibling, to_ar, to_al, to_br, to_bl,
        (z_r, s), (z_l, s), (z_r + 1 - 2 * c, s), (z_l + 1 - 2 * c, s),
    ):
        pl.semaphore_signal(barrier, inc=1, device_id=peer, device_id_type=MESH)

    gload.wait()
    turned = gs[...]
    first, second = turned[0:16], turned[16:32]
    mine = jnp.where(c == 0, first, second)
    theirs = jnp.where(c == 0, second, first)
    pad = jnp.zeros((16, 128), BF)
    buf[c, b, a, 0:16, :] = jnp.concatenate([mine, pad], axis=1)
    buf[other, a, b, 0:16, :] = jnp.concatenate([theirs, pad], axis=1)
    for copy in loads:
        copy.wait()

    pl.semaphore_wait(barrier, 9)

    def remote(src, dst, send, recv, to):
        copy = pltpu.make_async_remote_copy(
            src_ref=src, dst_ref=dst, send_sem=send, recv_sem=recv, device_id=to, device_id_type=MESH)
        return copy

    def same(ref, send, recv, to):
        return remote(ref, ref, send, recv, to)

    class Gather:
        def __init__(self, g):
            self.g, self.used, self.sent = g, 0, []
            rows = pl.ds(GROUPS[g][0], GROUPS[g][1] - GROUPS[g][0])
            col = (a, a_l, a_r, a_2)
            row = (b, b_l, b_r, b_2)

            def piece(i, k, to, half=None):
                ref = buf.at[c, row[i], col[k], rows]
                if half is not None:
                    ref = ref.at[:, pl.ds(256 * half, 256)]
                n = self.used
                self.used += 1
                copy = same(ref, g_s.at[g, n], g_r.at[g, n], to)
                self.sent.append(copy)
                return copy

            self.p1 = [piece(0, 0, to_ar), piece(0, 0, to_al)]
            self.p1f = [piece(0, 1, to_ar, 0), piece(0, 2, to_al, 1)]
            self.p2 = [[piece(0, k, to_br), piece(0, k, to_bl)] for k in range(4)]
            self.p2f = [piece(1, 0, to_br), piece(2, 1, to_bl), piece(2, 2, to_bl), piece(1, 3, to_br)]
            self.dd = {(i, k): piece(i, k, sibling) for i in range(4) for k in range(4) if i or k}

        def send_p1(self):
            start(self.p1)

        def send_p2(self, *ks):
            for k in ks:
                start(self.p2[k])

        def got_p1(self):
            arrived(self.p1)
            start(self.p1f)
            start([self.dd[0, 1], self.dd[0, 2]])

        def got_p1f(self):
            arrived(self.p1f)
            start([self.dd[0, 3]])

        def got_p2(self, *ks):
            for k in ks:
                arrived(self.p2[k])
                start([self.p2f[k], self.dd[1, k], self.dd[2, k]])

        def got_p2f(self, *ks):
            for k in ks:
                arrived([self.p2f[k]])
                start([self.dd[3, k]])

        def done(self):
            arrived(self.dd.values())

    def start(copies):
        for copy in copies:
            copy.start()

    def arrived(copies):
        for copy in copies:
            copy.wait_recv()

    ga, gb, gc = Gather(0), Gather(1), Gather(2)

    ga.send_p1()
    ga.send_p2(0)
    gb.send_p1()
    gc.send_p1()
    for peer in (z_r, z_l):
        pl.semaphore_signal(near, inc=1, device_id=(peer, s), device_id_type=MESH)

    for copy in ins[0:6]:
        copy.wait()
    lanes = lax.broadcasted_iota(jnp.int32, (128, 128), 1).astype(F32)
    node_rows = lax.broadcasted_iota(jnp.int32, (256, 128), 0).astype(F32)

    def hot(col, first):
        return jnp.where(col == lanes + float(first), 1.0, 0.0).astype(BF)

    lsrc = lsrc_v[...].astype(F32)
    ltgt = ltgt_v[...].astype(F32)
    for j in range(4):
        col = column(lsrc[j:j + 1])
        for k in range(2):
            ol[128 * j:128 * (j + 1), 128 * k:128 * (k + 1)] = hot(col, 128 * k)
        col = column(ltgt[j:j + 1])
        for k in range(2):
            ol[128 * j:128 * (j + 1), 256 + 128 * k:256 + 128 * (k + 1)] = hot(col, 128 * k)
        olt[:, 128 * j:128 * (j + 1)] = jnp.where(node_rows == ltgt[j:j + 1], 1.0, 0.0).astype(BF)
    ga.got_p1()
    ga.send_p2(1, 2)
    ga.got_p2(0)
    gb.got_p1()

    snd = snd_v[...].astype(F32)
    rcv = rcv_v[...].astype(F32)

    def edge_hot(js):
        for j in js:
            at = slice(128 * j, 128 * (j + 1))
            col = column(snd[j:j + 1])
            for k in range(2):
                x_v[at, 512 + 128 * k:512 + 128 * (k + 1)] = hot(col, 128 * k)
            x_v[at, 1024:1152] = hot(col, 256)
            col = column(rcv[j:j + 1])
            for k in range(2):
                x_v[at, 768 + 128 * k:768 + 128 * (k + 1)] = hot(col, 128 * k)
            t, o = j // 4, 128 * (j % 4)
            ort[t, :, o:o + 128] = jnp.where(node_rows == rcv[j:j + 1], 1.0, 0.0).astype(BF)

    edge_hot(range(0, 8))
    for j in range(2):
        acol[128 * j:128 * (j + 1), :] = column(area_v[j:j + 1, :])
    ga.got_p1f()
    ga.send_p2(3)
    gb.send_p2(0)
    ga.got_p2(1, 2)
    gb.send_p2(1, 2)
    gc.got_p1()
    edge_hot(range(8, 16))
    ga.got_p2f(0)
    gb.got_p1f()
    ga.got_p2(3)
    gb.send_p2(3)
    gb.got_p2(0)
    gc.send_p2(0)
    pl.semaphore_wait(near, 2)
    for peer in (z_2r, z_2l):
        pl.semaphore_signal(far, inc=1, device_id=(peer, s), device_id_type=MESH)
    ga.got_p2f(1, 2, 3)
    gb.got_p2(1, 2)
    gc.send_p2(1, 2)

    def assemble(at, rows, put):
        for i in range(16):
            put(i * 2 * rows, buf[0, i // 4, i % 4, at:at + rows, :])
            put(i * 2 * rows + rows, buf[1, i % 4, i // 4, at:at + rows, :])

    ga.done()
    for i in range(16):
        gt_w[i * 32:i * 32 + 16, :] = buf[0, i // 4, i % 4, 0:16, 0:384]
        gt_w[i * 32 + 16:i * 32 + 32, :] = buf[1, i % 4, i // 4, 0:16, 0:384]

    def put_enc(at, block):
        enc_w[at:at + block.shape[0], :] = block

    assemble(ENC_AT, 32, put_enc)
    for copy in ins[6:9]:
        copy.wait()

    grid_latent = silu(lax.dot_general(
        gridf_v[...], gt_w[...], (((1,), (1,)), ((), ())), preferred_element_type=F32)).astype(BF)
    from_grid = dot(grid_latent, enc_w[0:512, :]).astype(BF)
    from_mesh = dot(mesh_v[...], enc_w[512:1024, :]).astype(BF)
    messages = silu(dot(ol[...], jnp.concatenate([from_grid, from_mesh], axis=0))).astype(BF)
    l0[...] = (mesh_v[...].astype(F32) + dot(olt[...], messages)).astype(BF)

    slot_rows = lax.broadcasted_iota(jnp.int32, (256, 32), 0)
    for d in range(4):
        pick = jnp.where(slot_rows == lists_v[d:d + 1, :], 1.0, 0.0).astype(BF)
        hs[d] = lax.dot_general(
            pick, l0[...], (((0,), (0,)), ((), ())), preferred_element_type=F32).astype(BF)
    targets = (
        (lax.rem(f + 1, 16), s), (lax.rem(f + 15, 16), s), (f, lax.rem(s + 1, 16)), (f, lax.rem(s + 15, 16)))
    halo = [remote(hs.at[d], hr.at[d], h_s.at[d], h_r.at[d], targets[d]) for d in range(4)]
    start(halo)
    gb.got_p2f(0)
    gc.got_p1f()
    gb.got_p2(3)
    gc.send_p2(3)
    gc.got_p2(0)
    gb.got_p2f(1, 2, 3)
    gb.done()
    gc.got_p2(1, 2)

    def put_ef(at, block):
        done = 0
        while done < block.shape[0]:
            place = at + done
            limit = block.shape[0] - done if place >= 512 else min(block.shape[0] - done, 512 - place)
            if place < 512:
                r_w[place:place + limit, :] = block[done:done + limit]
            else:
                w23[place - 512:place - 512 + limit, :] = block[done:done + limit]
            done += limit

    assemble(EF_AT, 48, put_ef)
    r_w[512:768, :] = dot(l0[...], w23[0:512, :]).astype(BF)
    r_w[768:1024, :] = dot(l0[...], w23[512:1024, :]).astype(BF)
    for t in range(4):
        at = slice(TILE * t, TILE * (t + 1))
        e1[at, :] = dot(x_v[at, 0:1024], r_w[0:1024, :])
        if t == 1:
            gc.got_p2f(0)
            gc.got_p2(3)
    arrived(halo)
    r_w[1024:1152, :] = dot(hr[...].reshape(128, 512), w23[0:512, :]).astype(BF)
    def put_to(ref):
        def put(at, block):
            ref[at:at + block.shape[0], :] = block
        return put

    assemble(ES_AT, 16, put_to(es_w))

    incoming = jnp.zeros((256, 512), F32)
    for t in range(4):
        at = slice(TILE * t, TILE * (t + 1))
        hidden = silu(e1[at, :] + dot(x_v[at, 1024:1152], r_w[1024:1152, :])).astype(BF)
        new = (x_v[at, 0:512].astype(F32) + dot(hidden, es_w[...])).astype(BF)
        edge_o[at, :] = new
        incoming = incoming + dot(ort[t], new)
        if t == 1:
            gc.got_p2f(1, 2)
        if t == 2:
            gc.got_p2f(3)
    gc.done()
    assemble(NF_AT, 32, put_to(nf_w))
    assemble(NS_AT, 16, put_to(ns_w))

    node_hidden = silu(dot(l0[...], nf_w[0:512, :]) + dot(incoming.astype(BF), nf_w[512:1024, :])).astype(BF)
    result = (l0[...].astype(F32) + dot(node_hidden, ns_w[...])).astype(BF)
    mesh_o[...] = result

    wide = result.astype(F32)
    for k in range(4):
        msrc[:, 128 * k:128 * (k + 1)] = jnp.sum(wide[:, 128 * k:128 * (k + 1)] * acol[...], axis=0, keepdims=True)

    def exchange(source, slots, me, peer, sends, recvs):
        slots[me] = source[...]
        copies = [
            remote(source, slots.at[me], sends.at[k - 1], recvs.at[me], peer(lax.rem(me + k, 16)))
            for k in range(1, 16)
        ]
        start(copies)
        for k in range(1, 16):
            j = lax.rem(me + k, 16)
            remote(source, slots.at[j], sends.at[k - 1], recvs.at[j], peer(j)).wait_recv()
        return copies

    pl.semaphore_wait(far, 2)
    by_sub = exchange(msrc, asub, s, lambda j: (f, j), ms_s, ms_r)
    fsrc[...] = jnp.sum(asub[...], axis=0)
    by_face = exchange(fsrc, aface, f, lambda j: (j, s), mf_s, mf_r)
    total = jnp.sum(aface[...], axis=0) / 65536.0
    mass_o[...] = total

    for group in (ga.sent, gb.sent, gc.sent, halo, by_sub, by_face):
        for copy in group:
            copy.wait_send()


def per_device(
    mesh_latent, edge_latent, grid_features, senders, receivers, send_lists, link_sources, link_targets,
    node_area, grid_weight, encode_weight, edge_first, edge_second, node_first, node_second,
):
    dma = pltpu.SemaphoreType.DMA
    vm = pltpu.VMEM
    operands = (
        mesh_latent, edge_latent, grid_features, senders.reshape(16, 128), receivers.reshape(16, 128),
        send_lists[0], link_sources.reshape(4, 128), link_targets.reshape(4, 128), node_area.reshape(2, 128),
        grid_weight.T, encode_weight, edge_first[0], edge_second[0], node_first[0], node_second[0],
    )
    return pl.pallas_call(
        kernel,
        out_shape=(
            pltpu.VMEM((256, 512), BF),
            pltpu.VMEM((2048, 512), BF),
            pltpu.VMEM((1, 512), F32),
        ),
        in_specs=[pl.BlockSpec(memory_space=pltpu.HBM)] * 15,
        out_specs=(
            pl.BlockSpec(memory_space=pltpu.VMEM),
            pl.BlockSpec(memory_space=pltpu.VMEM),
            pl.BlockSpec(memory_space=pltpu.VMEM),
        ),
        scratch_shapes=[
            vm((2, 4, 4, ROWS, 512), BF), vm((32, 384), BF), vm((256, 512), BF), vm((256, 384), BF),
            vm((2048, 1152), BF), vm((16, 128), jnp.int32), vm((16, 128), jnp.int32), vm((4, 32), jnp.int32),
            vm((4, 128), jnp.int32), vm((4, 128), jnp.int32), vm((2, 128), F32),
            vm((512, 384), BF), vm((1024, 512), BF), vm((1152, 512), BF), vm((1024, 512), BF),
            vm((512, 512), BF), vm((1024, 512), BF), vm((512, 512), BF),
            vm((512, 512), BF), vm((256, 512), BF), vm((4, 256, 512), BF), vm((2048, 512), F32),
            vm((256, 512), BF), vm((4, 32, 512), BF), vm((4, 32, 512), BF), vm((256, 128), F32), vm((1, 512), F32), vm((16, 1, 512), F32),
            vm((1, 512), F32), vm((16, 1, 512), F32),
            dma((9,)), dma((11,)), dma((3, PIECES)), dma((3, PIECES)),
            pltpu.SemaphoreType.REGULAR, pltpu.SemaphoreType.REGULAR, dma((4,)), dma((4,)),
            dma((15,)), dma((16,)), dma((15,)), dma((16,)),
        ],
        compiler_params=pltpu.CompilerParams(
            collective_id=0, has_side_effects=True, vmem_limit_bytes=40 * 1024 * 1024),
        cost_estimate=pl.CostEstimate(flops=6_000_000_000, bytes_accessed=6_000_000, transcendentals=1_500_000),
        name="graph_layer",
    )(*(pltpu.with_memory_space_constraint(operand, pltpu.HBM) for operand in operands))


def solution(mesh):
    both = ("face", "sub")
    placed = (
        P(both, None), P(both, None), P(both, None), P(both), P(both), P(both, None, None), P(both), P(both), P(both),
        P(None, "sub"), P("sub", None), P(None, "sub", None), P(None, "sub", None), P(None, "sub", None),
        P(None, "sub", None),
    )
    return jax.shard_map(
        per_device, mesh=mesh, in_specs=placed, out_specs=(P(both, None), P(both, None), P()), check_vma=False)
```
